32 devices in a mesh: ma: 8 (over y, x, core), lev: 4 (over z).
Axes of the slice: x: 2, y: 2, z: 4, core: 2. Of those that a mesh axis runs over, the one named last changes fastest.
Arguments:
- spectral_state: float32 [1280, 2, 16, 1280], P('ma', None, None, 'lev'), may hold values from -6 to 6
- forcing_noise: bfloat16 [1280, 2, 16, 1280], P('ma', None, None, 'lev'), may hold values from -6 to 6
- decay_rate: float32 [16], replicated, may hold values from 0.3 to 0.95
- amplitude: float32 [1280], P('lev'), may hold values from 0.2 to 2
- legendre: bfloat16 [1280, 1280, 640], P('ma', 'lev'), may hold values from -0.0048828125 to 0.0048828125
- wave_of_slot: int32 [1280], replicated, may hold values from 0 to 1279, each once
- lat_of_row: int32 [1280], replicated, may hold values from 0 to 1279, each once
Outputs:
- new_state: float32 [1280, 2, 16, 1280], P('ma', None, None, 'lev')
- pattern: bfloat16 [16, 1280, 2560], P('lev', 'ma')
The draws below stay inside these ranges and needn't reach their ends.
Inputs may be any that keep to these rules, and one draw needn't show every extreme that they name: `wave_of_slot`: each zonal wavenumber is held by exactly one slot. `lat_of_row`: each latitude is held by exactly one row.
All inputs are finite; a program needn't handle non-finite values.
Results may differ from the reference program's by a relative error of at most 0.014.
Values may be sent and summed in bfloat16 or wider, within the bound.
No kernel may reach another device: no remote copies, remote signals or barrier semaphores. Data moves between devices by JAX's collectives and lax.ppermute only.
A program may use at most 192 MiB of HBM per device.

```python
import math
import jax
import jax.numpy as jnp
from jax import lax

M = 1280
N = 1280
NLAT = 1280
NLON = 2560
LEVELS = 16
N_LEV = 4


def levels(own_key, dims, pieces, smallest, top_value):
    level = 1.0
    for axis_at, parts in pieces:
        draws = jax.random.uniform(jax.random.fold_in(jax.random.fold_in(own_key, 6), axis_at), (parts,), jnp.float32, smallest / len(pieces), top_value / len(pieces))
        level = level * jnp.repeat(jnp.exp(draws), dims[axis_at] // parts).reshape((-1,) + (1,) * (len(dims) - 1 - axis_at))
    return level


def normal_values(stream_key, shape, spread, most, cuts=(), kind=jnp.bfloat16):
    array = spread * jax.random.normal(stream_key, shape, jnp.float32)
    if cuts:
        array = array * levels(stream_key, shape, cuts, -0.22, 0.18)
    return jnp.clip(array, -most, most).astype(kind)


def setup_inputs(seed: int = 0) -> dict:
    key_list = jax.random.split(jax.random.key(seed), 8)
    return {
        "spectral_state": normal_values(key_list[0], (M, 2, LEVELS, N), 1.0, 6.0, ((0, 8), (3, 4)), jnp.float32),
        "forcing_noise": normal_values(key_list[1], (M, 2, LEVELS, N), 1.0, 6.0, ((0, 8), (3, 4))),
        "decay_rate": jnp.clip(jnp.exp(jax.random.uniform(key_list[2], (LEVELS,), jnp.float32, math.log(0.3), math.log(0.95))), 0.3, 0.95),
        "amplitude": jnp.clip(jnp.exp(math.log(2.0) - 2.3025851 * jax.random.uniform(key_list[3], (N,), jnp.float32) ** levels(key_list[3], (N,), ((0, 4),), -0.2, 0.2)), 0.2, 2.0),
        "legendre": normal_values(key_list[4], (M, N, NLAT // 2), (N * M) ** -0.5, 0.0048828125, ((0, 8), (1, 4))),
        "wave_of_slot": jax.random.permutation(key_list[5], M).astype(jnp.int32),
        "lat_of_row": jax.random.permutation(key_list[6], NLAT).astype(jnp.int32),
    }


def build_table(wavenum, width):
    column = jnp.arange(width, dtype=jnp.int32)
    product = (wavenum[:, None] * column[None, :]) % width
    phase_angle = product.astype(jnp.float32) * jnp.float32(2.0 * math.pi / width)
    factor = jnp.where(wavenum == 0, jnp.float32(1.0), jnp.float32(2.0))[:, None]
    stacked = jnp.stack([factor * jnp.cos(phase_angle), -factor * jnp.sin(phase_angle)], axis=1)
    return stacked.astype(jnp.bfloat16)


def reference(spectral_state, forcing_noise, decay_rate, amplitude, legendre, wave_of_slot, lat_of_row):
    wavenum = wave_of_slot.astype(jnp.int32)
    total_n = jnp.arange(N, dtype=jnp.int32)
    valid_mask = total_n[None, :] >= wavenum[:, None]
    updated = decay_rate[None, None, :, None] * spectral_state + amplitude[None, None, None, :] * forcing_noise.astype(jnp.float32)
    new_state = jnp.where(valid_mask[:, None, None, :], updated, jnp.float32(0.0))
    spectral = new_state.astype(jnp.bfloat16)
    odd_mask = ((total_n[None, :] - wavenum[:, None]) % 2) == 1
    block_len = N // N_LEV
    running = jnp.zeros((M, 2 * LEVELS, NLAT), jnp.float32)
    for block_index in range(N_LEV):
        lower = block_index * block_len
        piece = spectral[:, :, :, lower:lower + block_len].reshape(M, 2 * LEVELS, block_len)
        odd_block = odd_mask[:, None, lower:lower + block_len]
        even_part = jnp.where(odd_block, jnp.zeros_like(piece), piece)
        odd_part = jnp.where(odd_block, piece, jnp.zeros_like(piece))
        stacked = jnp.concatenate([even_part, odd_part], axis=1).astype(jnp.float32)
        weights = legendre[:, lower:lower + block_len, :].astype(jnp.float32)
        halves = jnp.einsum("scn,snj->scj", stacked, weights)
        even_sum = halves[:, :2 * LEVELS]
        odd_sum = halves[:, 2 * LEVELS:]
        full = jnp.concatenate([even_sum + odd_sum, jnp.flip(even_sum - odd_sum, axis=2)], axis=2)
        rounded = lax.optimization_barrier(full.astype(jnp.bfloat16))
        running = running + rounded.astype(jnp.float32)
    fourier = running.reshape(M, 2, LEVELS, NLAT).astype(jnp.bfloat16)
    by_row = jnp.take(fourier, lat_of_row.astype(jnp.int32), axis=3)
    dft_table = build_table(wavenum, NLON)
    pattern = jnp.einsum("srlk,srx->lkx", by_row.astype(jnp.float32), dft_table.astype(jnp.float32))
    return new_state, pattern.astype(jnp.bfloat16)
```

```python
import functools
import math

import jax
import jax.numpy as jnp
from jax import lax
from jax.experimental import pallas as pl
from jax.experimental.pallas import tpu as pltpu
from jax.sharding import PartitionSpec as P


MIB = 2**20
TAIL, HEAD = (0, 1), (2, 3)


def table_kernel(width, wave, out):
    count = wave.shape[1]
    number = wave[0]
    column = lax.broadcasted_iota(jnp.int32, (count, 128), 1)
    scale = jnp.float32(2.0 * math.pi / width)

    def angle(product):
        real = product.astype(jnp.float32)
        turns = (real * jnp.float32(1.0 / width)).astype(jnp.int32)
        return (product - turns * width).astype(jnp.float32) * scale

    fine = angle(number * column)
    coarse = angle(number * (column * 128))
    factor = jnp.where(number == 0, 1.0, 2.0).astype(jnp.float32)
    fine_cos, fine_sin = factor * jnp.cos(fine), factor * jnp.sin(fine)
    coarse_cos, coarse_sin = jnp.cos(coarse), jnp.sin(coarse)
    for t in range(width // 128):
        c, s = coarse_cos[:, t : t + 1], coarse_sin[:, t : t + 1]
        lanes = pl.ds(t * 128, 128)
        out[0, pl.ds(0, count), lanes] = (c * fine_cos - s * fine_sin).astype(out.dtype)
        out[0, pl.ds(count, count), lanes] = -(s * fine_cos + c * fine_sin).astype(out.dtype)


def table_group(wavenum, width):
    owners, count = wavenum.shape
    wide = jnp.broadcast_to(wavenum[:, :, None], (owners, count, 128))
    return pl.pallas_call(
        functools.partial(table_kernel, width),
        grid=(owners,),
        in_specs=[pl.BlockSpec((1, count, 128), lambda s: (s, 0, 0))],
        out_specs=pl.BlockSpec((1, 2 * count, width), lambda s: (s, 0, 0)),
        out_shape=jax.ShapeDtypeStruct((owners, 2 * count, width), jnp.bfloat16),
        cost_estimate=pl.CostEstimate(
            flops=16 * owners * count * width,
            bytes_accessed=4 * owners * count * width,
            transcendentals=0,
        ),
        name="table",
    )(wide)


def legendre_kernel(first, slots, n_lev, lv, chained, wave, rate, amp, state, noise, leg, *rest):
    if chained:
        rest = rest[1:]
    new_state, pieces, (far, decay, turn) = rest[0], rest[1:-3], rest[-3:]
    step = pl.program_id(0)
    block, width = state.shape[0], state.shape[3]
    half = leg.shape[2]
    dev = lax.axis_index("lev")
    lead_slot = lax.axis_index("ma") * slots + first + step * block
    rows = 2 * lv

    @pl.when(step == 0)
    def _():
        for l in range(n_lev * lv):
            decay[pl.ds(l, 1), :] = jnp.full((1, width), rate[l], jnp.float32)

    total_n = lax.broadcasted_iota(jnp.int32, (1, width), 1) + dev * width
    gain = amp[...].reshape(1, width)
    signs = []
    for i in range(block):
        offset = total_n - wave[lead_slot + i]
        valid = offset >= 0
        signs.append(jnp.where((offset & 1) == 1, -1.0, 1.0).astype(jnp.float32))
        parts = []
        for p in range(2):
            value = decay[...] * state[i, p] + gain * noise[i, p].astype(jnp.float32)
            value = jnp.where(valid, value, 0.0)
            new_state[i, p] = value
            parts.append(value)
        order = jnp.concatenate(
            [parts[p][j * lv : (j + 1) * lv] for j in range(n_lev) for p in range(2)], axis=0
        )
        turn[i, pl.ds(0, n_lev * rows), :] = order
        turn[i, pl.ds(n_lev * rows, n_lev * rows), :] = order
    lead = pl.multiple_of(dev * rows, rows)
    held = []
    for i in range(block):
        coeff = turn[i, pl.ds(lead, n_lev * rows), :]
        lhs = jnp.concatenate([coeff, coeff * signs[i]], axis=0).astype(jnp.bfloat16)
        held.append(jnp.dot(lhs, leg[i], preferred_element_type=jnp.float32))
        if i % 2 == 1:
            for k in range(n_lev):
                at = pl.ds((i - 1) * rows, 2 * rows)
                for side in range(2):
                    base = side * n_lev * rows + k * rows
                    pair = jnp.concatenate([h[base : base + rows] for h in held], axis=0)
                    pair = pair.astype(jnp.bfloat16)
                    pieces[k][at, pl.ds(side * half, half)] = pair
                    if k in (1, n_lev - 1):

                        @pl.when((k == 1) == (dev == n_lev - 1))
                        def _():
                            far[at, pl.ds(side * half, half)] = pair

            held = []


def legendre_group(first, count, n_lev, wave, rate, amp, state, noise, leg, chain):
    slots, _, level_count, width = state.shape
    half = leg.shape[2]
    lv = level_count // n_lev
    rows = 2 * lv
    sb = next(b for b in (16, 8, 4, 2) if first % b == 0 and count % (2 * b) in (0, b) and count > b)
    base = first // sb
    chained = chain is not None
    four = lambda s, *_: (base + s, 0, 0, 0)
    in_specs = [
        pl.BlockSpec((width,), lambda s, *_: (0,)),
        pl.BlockSpec((sb, 2, level_count, width), four),
        pl.BlockSpec((sb, 2, level_count, width), four),
        pl.BlockSpec((sb, width, half), lambda s, *_: (base + s, 0, 0)),
    ]
    args = [wave, rate, amp, state, noise, leg]
    if chained:
        in_specs.append(pl.BlockSpec(memory_space=pl.ANY))
        args.append(chain)
    out = pl.pallas_call(
        functools.partial(legendre_kernel, first, slots, n_lev, lv, chained),
        grid_spec=pltpu.PrefetchScalarGridSpec(
            num_scalar_prefetch=2,
            grid=(count // sb,),
            in_specs=in_specs,
            out_specs=[pl.BlockSpec((sb, 2, level_count, width), four)]
            + [pl.BlockSpec((sb * rows, 2 * half), lambda s, *_: (s, 0))] * (n_lev + 1),
            scratch_shapes=[
                pltpu.VMEM((level_count, width), jnp.float32),
                pltpu.VMEM((sb, 2 * n_lev * rows, width), jnp.float32),
            ],
        ),
        out_shape=[jax.ShapeDtypeStruct(state.shape, jnp.float32)]
        + [jax.ShapeDtypeStruct((count * rows, 2 * half), jnp.bfloat16)] * (n_lev + 1),
        input_output_aliases={6: 0} if chained else {},
        cost_estimate=pl.CostEstimate(
            flops=4 * count * n_lev * rows * width * half,
            bytes_accessed=count * width * (half * 2 + 10 * n_lev * rows),
            transcendentals=0,
        ),
    )(*args)
    return out[0], out[1:]


def rows_kernel(lv, *refs):
    addends, (pick, out, total, ready) = refs[:-4], refs[-4:]
    own = addends[0]
    rows = 2 * lv
    count = own.shape[0] // rows
    owners, per, chunk = out.shape

    @pl.when(pl.program_id(0) == 0)
    def _():
        for t in range(own.shape[1] // 128):
            lanes = pl.ds(t * 128, 128)
            value = own[:, lanes].astype(jnp.float32)
            for other in addends[1:]:
                value = value + other[:, lanes].astype(jnp.float32)
            total[t] = value
            for l in range(lv):
                for p in range(2):
                    some = total[t, pl.ds(p * lv + l, count, stride=rows), :]
                    ready[pl.ds((2 * l + p) * count, count), lanes] = some.astype(jnp.bfloat16)

    mine = ready[pl.ds(pl.multiple_of(pl.program_id(0) * chunk, chunk), chunk), :]
    out[...] = (
        lax.dot_general(
            pick[...], mine, (((1,), (1,)), ((), ())), preferred_element_type=jnp.float32
        )
        .astype(jnp.bfloat16)
        .reshape(owners, per, chunk)
    )


def rows_group(n_ma, lv, addends, pick):
    own = addends[0]
    lat_count = pick.shape[0]
    per = lat_count // n_ma
    n_rows = own.shape[0]
    chunk = 256 if n_rows % 256 == 0 else n_rows
    whole = pl.BlockSpec(own.shape, lambda s: (0, 0))
    return pl.pallas_call(
        functools.partial(rows_kernel, lv),
        grid=(n_rows // chunk,),
        in_specs=[whole] * len(addends) + [pl.BlockSpec(pick.shape, lambda s: (0, 0))],
        out_specs=pl.BlockSpec((n_ma, per, chunk), lambda s: (0, 0, s)),
        out_shape=jax.ShapeDtypeStruct((n_ma, per, n_rows), jnp.bfloat16),
        scratch_shapes=[
            pltpu.VMEM((own.shape[1] // 128, n_rows, 128), jnp.float32),
            pltpu.VMEM(own.shape, jnp.bfloat16),
        ],
        cost_estimate=pl.CostEstimate(
            flops=2 * n_rows * lat_count * lat_count,
            bytes_accessed=8 * n_rows * lat_count + 2 * lat_count * lat_count,
            transcendentals=0,
        ),
        compiler_params=pltpu.CompilerParams(vmem_limit_bytes=24 * MIB),
        name="rows",
    )(*addends, pick)


def wave_kernel(lv, counts, has_acc, *refs):
    total = sum(counts)
    tables = refs[total : total + len(counts)]
    end = total + len(counts) + has_acc
    out, lhs = refs[end], refs[end + 1 :]
    owners, per, _ = refs[0].shape

    @pl.when(pl.program_id(0) == 0)
    def _():
        at = 0
        for count, left in zip(counts, lhs):
            spectra = refs[at : at + count]
            at += count
            depth = spectra[0].shape[2] // lv
            for o in range(owners):
                value = spectra[0][o]
                if count > 1:
                    value = sum(x[o].astype(jnp.float32) for x in spectra).astype(value.dtype)
                for l in range(lv):
                    left[pl.ds(l * per, per), pl.ds(o * depth, depth)] = value[
                        :, l * depth : (l + 1) * depth
                    ]

    value = None
    for table, left in zip(tables, lhs):
        part = jnp.dot(
            left[...],
            table[...].reshape(left.shape[1], table.shape[2]),
            preferred_element_type=jnp.float32,
        )
        value = part if value is None else value + part
    value = value.reshape(out.shape)
    if has_acc:
        value = value + refs[end - 1][...]
    out[...] = value.astype(out.dtype)


def wave_group(lv, spectra, tables, acc, dtype):
    owners, per, _ = spectra[0][0].shape
    width = tables[0].shape[-1]
    xb = width // 5
    in_specs = [pl.BlockSpec(x.shape, lambda s: (0, 0, 0)) for xs in spectra for x in xs]
    in_specs += [pl.BlockSpec((owners, t.shape[1], xb), lambda s: (0, 0, s)) for t in tables]
    sheet = pl.BlockSpec((lv, per, xb), lambda s: (0, 0, s))
    added = [] if acc is None else [acc]
    depth = sum(owners * t.shape[1] for t in tables)
    return pl.pallas_call(
        functools.partial(wave_kernel, lv, tuple(len(xs) for xs in spectra), len(added)),
        grid=(width // xb,),
        in_specs=in_specs + [sheet] * len(added),
        out_specs=sheet,
        out_shape=jax.ShapeDtypeStruct((lv, per, width), dtype),
        scratch_shapes=[
            pltpu.VMEM((lv * per, owners * t.shape[1]), jnp.bfloat16) for t in tables
        ],
        cost_estimate=pl.CostEstimate(
            flops=2 * lv * per * depth * width,
            bytes_accessed=width * (2 * lv * per + 2 * depth),
            transcendentals=0,
        ),
        compiler_params=pltpu.CompilerParams(vmem_limit_bytes=60 * MIB),
        name="wave",
    )(*[x for xs in spectra for x in xs], *tables, *added)


def plan(slots):
    return [part * slots // 10 for part in (1, 2, 4, 3)]


def body(n_ma, n_lev, state, noise, decay_rate, amplitude, legendre, wave_of_slot, lat_of_row):
    slots, _, level_count, _ = state.shape
    half = legendre.shape[2]
    lat_count = lat_of_row.shape[0]
    lv = level_count // n_lev
    sizes = plan(slots)
    firsts = [sum(sizes[:g]) for g in range(len(sizes))]
    groups = list(range(len(sizes)))

    chain = None
    pieces = []
    for g in groups:
        chain, out = legendre_group(
            firsts[g], sizes[g], n_lev, wave_of_slot, decay_rate, amplitude,
            state, noise, legendre, chain,
        )
        pieces.append(out)

    column = jnp.where(lat_of_row < half, lat_of_row, 3 * half - 1 - lat_of_row)
    number = jnp.arange(lat_count, dtype=jnp.int32)
    pick = (column[:, None] == number[None, :]).astype(jnp.bfloat16)

    def exchange(addends):
        spectrum = rows_group(n_ma, lv, addends, pick)
        return lax.all_to_all(spectrum, "ma", split_axis=0, concat_axis=0, tiled=True)

    def send(value, pairs):
        return lax.ppermute(value, "lev", pairs)

    from_above = [None] * len(sizes)
    from_below = [None] * len(sizes)
    for phase in range(n_lev - 1):
        last = phase == n_lev - 2
        dist = n_lev - 1 - phase
        down = [(i, i - 1) for i in range(dist, n_lev)]
        up = [(i, i + 1) for i in range(n_lev - dist)]
        lows, highs = {}, {}
        for g in groups:
            if phase == 0:
                from_above[g] = send(pieces[g][n_lev], down + up)
                from_below[g] = from_above[g]
                continue
            lows[g] = pieces[g][n_lev - dist] + from_above[g]
            highs[g] = pieces[g][dist] + from_below[g]
            if not last:
                from_above[g] = send(lows[g], down)
                from_below[g] = send(highs[g], up)
    for g in HEAD:
        from_above[g] = send(lows[g], down)
        from_below[g] = send(highs[g], up)
    join = lambda xs: jnp.concatenate([xs[g] for g in TAIL], axis=0)
    tail_own = exchange([join({g: pieces[g][0] for g in TAIL})])
    tail_low = exchange([join(lows)])
    tail_high = exchange([join(highs)])
    tail_low = send(tail_low, down)
    tail_high = send(tail_high, up)

    by_owner = wave_of_slot.reshape(n_ma, slots)
    spectra, tables = [], []
    for g in HEAD:
        spectra.append([exchange([pieces[g][0], from_above[g], from_below[g]])])
        tables.append(
            table_group(by_owner[:, firsts[g] : firsts[g] + sizes[g]], 2 * lat_count)
        )
    spectra.append([tail_own, tail_low, tail_high])
    tables.append(table_group(by_owner[:, : firsts[HEAD[0]]], 2 * lat_count))
    late = len(HEAD) - 1
    rest = [q for q in range(len(spectra)) if q != late]
    acc = wave_group(lv, [spectra[q] for q in rest], [tables[q] for q in rest], None, jnp.float32)
    pattern = wave_group(lv, [spectra[late]], [tables[late]], acc, jnp.bfloat16)
    return chain, pattern


def solution(mesh):
    n_lev = mesh.shape["lev"]

    def inner(*args):
        return body(mesh.shape["ma"], n_lev, *args)

    return jax.shard_map(
        inner,
        mesh=mesh,
        in_specs=(
            P("ma", None, None, "lev"),
            P("ma", None, None, "lev"),
            P(),
            P("lev"),
            P("ma", "lev", None),
            P(),
            P(),
        ),
        out_specs=(P("ma", None, None, "lev"), P("lev", "ma", None)),
        check_vma=False,
    )
```

```python
import functools
import math

import jax
import jax.numpy as jnp
from jax import lax
from jax.experimental import pallas as pl
from jax.experimental.pallas import tpu as pltpu
from jax.sharding import PartitionSpec as P


MIB = 2**20
TAIL, HEAD = (0, 1), (2, 3)


def table_kernel(width, wave, out):
    count = wave.shape[1]
    number = wave[0]
    column = lax.broadcasted_iota(jnp.int32, (count, 128), 1)
    scale = jnp.float32(2.0 * math.pi / width)

    def angle(product):
        real = product.astype(jnp.float32)
        turns = (real * jnp.float32(1.0 / width)).astype(jnp.int32)
        return (product - turns * width).astype(jnp.float32) * scale

    fine = angle(number * column)
    coarse = angle(number * (column * 128))
    factor = jnp.where(number == 0, 1.0, 2.0).astype(jnp.float32)
    fine_cos, fine_sin = factor * jnp.cos(fine), factor * jnp.sin(fine)
    coarse_cos, coarse_sin = jnp.cos(coarse), jnp.sin(coarse)
    for t in range(width // 128):
        c, s = coarse_cos[:, t : t + 1], coarse_sin[:, t : t + 1]
        lanes = pl.ds(t * 128, 128)
        out[0, pl.ds(0, count), lanes] = (c * fine_cos - s * fine_sin).astype(out.dtype)
        out[0, pl.ds(count, count), lanes] = -(s * fine_cos + c * fine_sin).astype(out.dtype)


def table_group(wavenum, width):
    owners, count = wavenum.shape
    wide = jnp.broadcast_to(wavenum[:, :, None], (owners, count, 128))
    return pl.pallas_call(
        functools.partial(table_kernel, width),
        grid=(owners,),
        in_specs=[pl.BlockSpec((1, count, 128), lambda s: (s, 0, 0))],
        out_specs=pl.BlockSpec((1, 2 * count, width), lambda s: (s, 0, 0)),
        out_shape=jax.ShapeDtypeStruct((owners, 2 * count, width), jnp.bfloat16),
        cost_estimate=pl.CostEstimate(
            flops=16 * owners * count * width,
            bytes_accessed=4 * owners * count * width,
            transcendentals=0,
        ),
        name="table",
    )(wide)


def legendre_kernel(first, slots, n_lev, lv, chained, wave, rate, amp, state, noise, leg, *rest):
    if chained:
        rest = rest[1:]
    new_state, pieces, (far, decay, turn) = rest[0], rest[1:-3], rest[-3:]
    step = pl.program_id(0)
    block, width = state.shape[0], state.shape[3]
    half = leg.shape[2]
    dev = lax.axis_index("lev")
    lead_slot = lax.axis_index("ma") * slots + first + step * block
    rows = 2 * lv

    @pl.when(step == 0)
    def _():
        for l in range(n_lev * lv):
            decay[pl.ds(l, 1), :] = jnp.full((1, width), rate[l], jnp.float32)

    total_n = lax.broadcasted_iota(jnp.int32, (1, width), 1) + dev * width
    gain = amp[...].reshape(1, width)
    signs = []
    for i in range(block):
        offset = total_n - wave[lead_slot + i]
        valid = offset >= 0
        signs.append(jnp.where((offset & 1) == 1, -1.0, 1.0).astype(jnp.float32))
        parts = []
        for p in range(2):
            value = decay[...] * state[i, p] + gain * noise[i, p].astype(jnp.float32)
            value = jnp.where(valid, value, 0.0)
            new_state[i, p] = value
            parts.append(value)
        order = jnp.concatenate(
            [parts[p][j * lv : (j + 1) * lv] for j in range(n_lev) for p in range(2)], axis=0
        )
        turn[i, pl.ds(0, n_lev * rows), :] = order
        turn[i, pl.ds(n_lev * rows, n_lev * rows), :] = order
    lead = pl.multiple_of(dev * rows, rows)
    held = []
    for i in range(block):
        coeff = turn[i, pl.ds(lead, n_lev * rows), :]
        lhs = jnp.concatenate([coeff, coeff * signs[i]], axis=0).astype(jnp.bfloat16)
        held.append(jnp.dot(lhs, leg[i], preferred_element_type=jnp.float32))
        if i % 2 == 1:
            for k in range(n_lev):
                at = pl.ds((i - 1) * rows, 2 * rows)
                for side in range(2):
                    base = side * n_lev * rows + k * rows
                    pair = jnp.concatenate([h[base : base + rows] for h in held], axis=0)
                    pair = pair.astype(jnp.bfloat16)
                    pieces[k][at, pl.ds(side * half, half)] = pair
                    if k in (1, n_lev - 1):

                        @pl.when((k == 1) == (dev == n_lev - 1))
                        def _():
                            far[at, pl.ds(side * half, half)] = pair

            held = []


def legendre_group(first, count, n_lev, wave, rate, amp, state, noise, leg, chain):
    slots, _, level_count, width = state.shape
    half = leg.shape[2]
    lv = level_count // n_lev
    rows = 2 * lv
    sb = next(b for b in (16, 8, 4, 2) if first % b == 0 and count % (2 * b) in (0, b) and count > b)
    base = first // sb
    chained = chain is not None
    four = lambda s, *_: (base + s, 0, 0, 0)
    in_specs = [
        pl.BlockSpec((width,), lambda s, *_: (0,)),
        pl.BlockSpec((sb, 2, level_count, width), four),
        pl.BlockSpec((sb, 2, level_count, width), four),
        pl.BlockSpec((sb, width, half), lambda s, *_: (base + s, 0, 0)),
    ]
    args = [wave, rate, amp, state, noise, leg]
    if chained:
        in_specs.append(pl.BlockSpec(memory_space=pl.ANY))
        args.append(chain)
    out = pl.pallas_call(
        functools.partial(legendre_kernel, first, slots, n_lev, lv, chained),
        grid_spec=pltpu.PrefetchScalarGridSpec(
            num_scalar_prefetch=2,
            grid=(count // sb,),
            in_specs=in_specs,
            out_specs=[pl.BlockSpec((sb, 2, level_count, width), four)]
            + [pl.BlockSpec((sb * rows, 2 * half), lambda s, *_: (s, 0))] * (n_lev + 1),
            scratch_shapes=[
                pltpu.VMEM((level_count, width), jnp.float32),
                pltpu.VMEM((sb, 2 * n_lev * rows, width), jnp.float32),
            ],
        ),
        out_shape=[jax.ShapeDtypeStruct(state.shape, jnp.float32)]
        + [jax.ShapeDtypeStruct((count * rows, 2 * half), jnp.bfloat16)] * (n_lev + 1),
        input_output_aliases={6: 0} if chained else {},
        cost_estimate=pl.CostEstimate(
            flops=4 * count * n_lev * rows * width * half,
            bytes_accessed=count * width * (half * 2 + 10 * n_lev * rows),
            transcendentals=0,
        ),
    )(*args)
    return out[0], out[1:]


def rows_kernel(lv, *refs):
    addends, (pick, out, total, ready) = refs[:-4], refs[-4:]
    own = addends[0]
    rows = 2 * lv
    count = own.shape[0] // rows
    owners, per, chunk = out.shape

    @pl.when(pl.program_id(0) == 0)
    def _():
        for t in range(own.shape[1] // 128):
            lanes = pl.ds(t * 128, 128)
            value = own[:, lanes].astype(jnp.float32)
            for other in addends[1:]:
                value = value + other[:, lanes].astype(jnp.float32)
            total[t] = value
            for l in range(lv):
                for p in range(2):
                    some = total[t, pl.ds(p * lv + l, count, stride=rows), :]
                    ready[pl.ds((2 * l + p) * count, count), lanes] = some.astype(jnp.bfloat16)

    mine = ready[pl.ds(pl.multiple_of(pl.program_id(0) * chunk, chunk), chunk), :]
    out[...] = (
        lax.dot_general(
            pick[...], mine, (((1,), (1,)), ((), ())), preferred_element_type=jnp.float32
        )
        .astype(jnp.bfloat16)
        .reshape(owners, per, chunk)
    )


def rows_group(n_ma, lv, addends, pick):
    own = addends[0]
    lat_count = pick.shape[0]
    per = lat_count // n_ma
    n_rows = own.shape[0]
    chunk = 256 if n_rows % 256 == 0 else n_rows
    whole = pl.BlockSpec(own.shape, lambda s: (0, 0))
    return pl.pallas_call(
        functools.partial(rows_kernel, lv),
        grid=(n_rows // chunk,),
        in_specs=[whole] * len(addends) + [pl.BlockSpec(pick.shape, lambda s: (0, 0))],
        out_specs=pl.BlockSpec((n_ma, per, chunk), lambda s: (0, 0, s)),
        out_shape=jax.ShapeDtypeStruct((n_ma, per, n_rows), jnp.bfloat16),
        scratch_shapes=[
            pltpu.VMEM((own.shape[1] // 128, n_rows, 128), jnp.float32),
            pltpu.VMEM(own.shape, jnp.bfloat16),
        ],
        cost_estimate=pl.CostEstimate(
            flops=2 * n_rows * lat_count * lat_count,
            bytes_accessed=8 * n_rows * lat_count + 2 * lat_count * lat_count,
            transcendentals=0,
        ),
        compiler_params=pltpu.CompilerParams(vmem_limit_bytes=24 * MIB),
        name="rows",
    )(*addends, pick)


def wave_kernel(lv, counts, has_acc, *refs):
    total = sum(counts)
    tables = refs[total : total + len(counts)]
    end = total + len(counts) + has_acc
    out, lhs = refs[end], refs[end + 1 :]
    owners, per, _ = refs[0].shape

    @pl.when(pl.program_id(0) == 0)
    def _():
        at = 0
        for count, left in zip(counts, lhs):
            spectra = refs[at : at + count]
            at += count
            depth = spectra[0].shape[2] // lv
            for o in range(owners):
                value = spectra[0][o]
                if count > 1:
                    value = sum(x[o].astype(jnp.float32) for x in spectra).astype(value.dtype)
                for l in range(lv):
                    left[pl.ds(l * per, per), pl.ds(o * depth, depth)] = value[
                        :, l * depth : (l + 1) * depth
                    ]

    value = None
    for table, left in zip(tables, lhs):
        part = jnp.dot(
            left[...],
            table[...].reshape(left.shape[1], table.shape[2]),
            preferred_element_type=jnp.float32,
        )
        value = part if value is None else value + part
    value = value.reshape(out.shape)
    if has_acc:
        value = value + refs[end - 1][...]
    out[...] = value.astype(out.dtype)


def wave_group(lv, spectra, tables, acc, dtype):
    owners, per, _ = spectra[0][0].shape
    width = tables[0].shape[-1]
    xb = width // 5
    in_specs = [pl.BlockSpec(x.shape, lambda s: (0, 0, 0)) for xs in spectra for x in xs]
    in_specs += [pl.BlockSpec((owners, t.shape[1], xb), lambda s: (0, 0, s)) for t in tables]
    sheet = pl.BlockSpec((lv, per, xb), lambda s: (0, 0, s))
    added = [] if acc is None else [acc]
    depth = sum(owners * t.shape[1] for t in tables)
    return pl.pallas_call(
        functools.partial(wave_kernel, lv, tuple(len(xs) for xs in spectra), len(added)),
        grid=(width // xb,),
        in_specs=in_specs + [sheet] * len(added),
        out_specs=sheet,
        out_shape=jax.ShapeDtypeStruct((lv, per, width), dtype),
        scratch_shapes=[
            pltpu.VMEM((lv * per, owners * t.shape[1]), jnp.bfloat16) for t in tables
        ],
        cost_estimate=pl.CostEstimate(
            flops=2 * lv * per * depth * width,
            bytes_accessed=width * (2 * lv * per + 2 * depth),
            transcendentals=0,
        ),
        compiler_params=pltpu.CompilerParams(vmem_limit_bytes=60 * MIB),
        name="wave",
    )(*[x for xs in spectra for x in xs], *tables, *added)


def plan(slots):
    return [part * slots // 10 for part in (1, 2, 4, 3)]


def body(n_ma, n_lev, state, noise, decay_rate, amplitude, legendre, wave_of_slot, lat_of_row):
    slots, _, level_count, _ = state.shape
    half = legendre.shape[2]
    lat_count = lat_of_row.shape[0]
    lv = level_count // n_lev
    sizes = plan(slots)
    firsts = [sum(sizes[:g]) for g in range(len(sizes))]
    groups = list(range(len(sizes)))

    chain = None
    pieces = []
    for g in groups:
        chain, out = legendre_group(
            firsts[g], sizes[g], n_lev, wave_of_slot, decay_rate, amplitude,
            state, noise, legendre, chain,
        )
        pieces.append(out)

    column = jnp.where(lat_of_row < half, lat_of_row, 3 * half - 1 - lat_of_row)
    number = jnp.arange(lat_count, dtype=jnp.int32)
    pick = (column[:, None] == number[None, :]).astype(jnp.bfloat16)

    def exchange(addends):
        spectrum = rows_group(n_ma, lv, addends, pick)
        return lax.all_to_all(spectrum, "ma", split_axis=0, concat_axis=0, tiled=True)

    def send(value, pairs):
        return lax.ppermute(value, "lev", pairs)

    from_above = [None] * len(sizes)
    from_below = [None] * len(sizes)
    for phase in range(n_lev - 1):
        last = phase == n_lev - 2
        dist = n_lev - 1 - phase
        down = [(i, i - 1) for i in range(dist, n_lev)]
        up = [(i, i + 1) for i in range(n_lev - dist)]
        lows, highs = {}, {}
        for g in groups:
            if phase == 0:
                from_above[g] = send(pieces[g][n_lev], down + up)
                from_below[g] = from_above[g]
                continue
            lows[g] = pieces[g][n_lev - dist] + from_above[g]
            highs[g] = pieces[g][dist] + from_below[g]
            if not last:
                from_above[g] = send(lows[g], down)
                from_below[g] = send(highs[g], up)
    for g in HEAD:
        from_above[g] = send(lows[g], down)
        from_below[g] = send(highs[g], up)
    join = lambda xs: jnp.concatenate([xs[g] for g in TAIL], axis=0)
    tail_own = exchange([join({g: pieces[g][0] for g in TAIL})])
    tail_low = exchange([join(lows)])
    tail_high = exchange([join(highs)])
    tail_low = send(tail_low, down)
    tail_high = send(tail_high, up)

    by_owner = wave_of_slot.reshape(n_ma, slots)
    spectra, tables = [], []
    for g in HEAD:
        spectra.append([exchange([pieces[g][0], from_above[g], from_below[g]])])
        tables.append(
            table_group(by_owner[:, firsts[g] : firsts[g] + sizes[g]], 2 * lat_count)
        )
    spectra.append([tail_own, tail_low, tail_high])
    tables.append(table_group(by_owner[:, : firsts[HEAD[0]]], 2 * lat_count))
    acc = wave_group(lv, spectra[:1], tables[:1], None, jnp.float32)
    pattern = wave_group(lv, spectra[1:], tables[1:], acc, jnp.bfloat16)
    return chain, pattern


def solution(mesh):
    n_lev = mesh.shape["lev"]

    def inner(*args):
        return body(mesh.shape["ma"], n_lev, *args)

    return jax.shard_map(
        inner,
        mesh=mesh,
        in_specs=(
            P("ma", None, None, "lev"),
            P("ma", None, None, "lev"),
            P(),
            P("lev"),
            P("ma", "lev", None),
            P(),
            P(),
        ),
        out_specs=(P("ma", None, None, "lev"), P("lev", "ma", None)),
        check_vma=False,
    )
```
